32 devices in a mesh: stage: 8 (over z, y), tp: 4 (over x, core).
Axes of the slice: x: 2, y: 2, z: 4, core: 2. Of those that a mesh axis runs over, the one named last changes fastest.
Arguments:
- x: bfloat16 [4, 512, 2048], P(None, 'tp')
- g: bfloat16 [8, 2, 2048], P('stage')
- w1: bfloat16 [8, 2, 2048, 8192], P('stage', None, None, 'tp')
- w2: bfloat16 [8, 2, 8192, 2048], P('stage', None, 'tp')
Outputs:
- output: bfloat16 [8, 4, 512, 2048], P('stage', None, 'tp')
All inputs are finite; a program needn't handle non-finite values.
Results may differ from the reference program's by a relative error of at most 0.02.
Values are sent between devices in bfloat16 or wider.
A program may use at most 1 GiB of HBM per device.

```python
import jax
import jax.numpy as jnp
from jax import lax

STAGES = 8
BLOCKS = 2
M = 4
T = 512
D = 2048
FF = 8192

EPS = 1e-5


def setup_inputs(seed: int = 0) -> dict:
    k = jax.random.split(jax.random.key(seed), 4)
    x = jax.random.normal(k[0], (M, T, D), jnp.float32)
    g = 1.0 + 0.2 * jax.random.normal(k[1], (STAGES, BLOCKS, D), jnp.float32)
    w1 = jax.random.normal(k[2], (STAGES, BLOCKS, D, FF), jnp.float32) * D ** -0.5
    w2 = jax.random.normal(k[3], (STAGES, BLOCKS, FF, D), jnp.float32) * FF ** -0.5
    return {'x': x.astype(jnp.bfloat16), 'g': g.astype(jnp.bfloat16),
            'w1': w1.astype(jnp.bfloat16), 'w2': w2.astype(jnp.bfloat16)}


def _block(y, g, w1, w2):
    yf = y.astype(jnp.float32)
    mu = jnp.mean(yf, axis=-1, keepdims=True)
    var = jnp.mean(jnp.square(yf - mu), axis=-1, keepdims=True)
    h = ((yf - mu) * lax.rsqrt(var + EPS) * g.astype(jnp.float32)).astype(jnp.bfloat16)
    a = jax.nn.gelu(jnp.dot(h, w1, preferred_element_type=jnp.float32)).astype(jnp.bfloat16)
    return (yf + jnp.dot(a, w2, preferred_element_type=jnp.float32)).astype(jnp.bfloat16)


def reference(x, g, w1, w2):
    def one(xm):
        y = xm
        outs = []
        for s in range(STAGES):
            for b in range(BLOCKS):
                y = _block(y, g[s, b], w1[s, b], w2[s, b])
            outs.append(y)
        return jnp.stack(outs)
    return jnp.transpose(lax.map(one, x), (1, 0, 2, 3))
```

```python
import functools

import jax
import jax.numpy as jnp
from jax import lax
from jax.experimental import pallas as pl
from jax.experimental.pallas import tpu as pltpu
from jax.sharding import PartitionSpec as P

EPS = 1e-5
CHUNK = 64
PIECES = 4
MESH = pl.DeviceIdType.MESH
F32, BF16 = jnp.float32, jnp.bfloat16


def _gelu(v):
    return 0.5 * v * (1.0 + jnp.tanh(0.7978845608028654 * (v + 0.044715 * (v * v * v))))


def _kernel(S, M, TL, x_ref, g_ref, w1_ref, w2_ref, out_ref, W1, W2, y, xr, p, h, a,
            w_sem, w_send, y_sem, y_send, x_sem, p_send, o_sem, o_send, in_send):
    C = CHUNK
    s, r = lax.axis_index('stage'), lax.axis_index('tp')
    xp, c = r // 2, r % 2
    sub_n = TL // C
    per_rank = M * sub_n
    N = 4 * per_rank
    D = h.shape[1]
    DP = D // PIECES
    H = W1.shape[2]
    TH = min(512, H)
    sib = (s, 2 * xp + 1 - c)
    partner = (s, 2 * (1 - xp) + c)
    succ = (s + c, 2 * xp + 1 - c)
    has_succ = 2 * s + c < 2 * S - 1

    def remote(src, dst, ss, rs, dev):
        return pltpu.make_async_remote_copy(src_ref=src, dst_ref=dst, send_sem=ss, recv_sem=rs,
                                            device_id=dev, device_id_type=MESH)

    own1 = pltpu.make_async_copy(w1_ref.at[0, c], W1.at[0], w_sem.at[0])
    own2 = pltpu.make_async_copy(w2_ref.at[0, c], W2.at[0], w_sem.at[2])
    sib1 = remote(w1_ref.at[0, 1 - c], W1.at[1], w_send.at[0], w_sem.at[1], sib)
    sib2 = remote(w2_ref.at[0, 1 - c], W2.at[1], w_send.at[1], w_sem.at[3], sib)
    own1.start()

    def x_piece(i, k):
        return x_ref.at[i // sub_n, pl.ds(pl.multiple_of((i % sub_n) * C, C), C), pl.ds(k * DP, DP)]

    def sender(i):
        return jnp.maximum(1, i * S // per_rank)

    @pl.when(s == 0)
    def _():
        @pl.loop(0, per_rank)
        def _(i):
            for k in range(PIECES):
                @pl.when(c == 0)
                def _():
                    pltpu.make_async_copy(x_piece(i, k), y.at[4 * i + r, k], y_sem.at[4 * i + r]).start()

                @pl.when(c == 1)
                def _():
                    remote(x_piece(i, k), y.at[4 * i + r, k], in_send.at[i], y_sem.at[4 * i + r], sib).start()

    @pl.when(s > 0)
    def _():
        @pl.loop(0, per_rank)
        def _(i):
            @pl.when(s == sender(i))
            def _():
                for k in range(PIECES):
                    remote(x_piece(i, k), y.at[4 * i + r, k], in_send.at[i], y_sem.at[4 * i + r],
                           (0, 2 * (1 - xp))).start()

    sib1.start()
    own2.start()
    sib2.start()

    g = jnp.where(c == 0, g_ref[0, 0:1, :].astype(F32), g_ref[0, 1:2, :].astype(F32))

    def p_copy(t, k):
        return remote(p.at[t % 2, k], xr.at[t, k], p_send.at[t % 2, k], x_sem.at[t, k], partner)

    def out_piece(t, k):
        i = t // 4
        return out_ref.at[0, i // sub_n, pl.ds(pl.multiple_of((i % sub_n) * C, C), C), pl.ds(k * DP, DP)]

    def finish(t, k):
        p_copy(t, k).wait()
        v = y[t, k].astype(F32) + (p[t % 2, k].astype(F32) + xr[t, k].astype(F32))
        y[t, k] = v.astype(BF16)

        @pl.when(has_succ)
        def _():
            remote(y.at[t, k], y.at[t, k], y_send.at[t], y_sem.at[t], succ).start()

        mine = (c == 1) & ((t % 4) // 2 == xp)

        @pl.when(mine & (t % 2 == 1))
        def _():
            pltpu.make_async_copy(y.at[t, k], out_piece(t, k), o_sem.at[t // 4]).start()

        @pl.when(mine & (t % 2 == 0))
        def _():
            remote(y.at[t, k], out_piece(t, k), o_send.at[t // 4], o_sem.at[t // 4], sib).start()

    def step(t, first):
        pltpu.make_async_copy(y.at[t], y.at[t], y_sem.at[t]).wait()
        tot = y[t, 0].astype(F32)
        for k in range(1, PIECES):
            tot = tot + y[t, k].astype(F32)
        mu = jnp.sum(tot, axis=-1, keepdims=True) * (1.0 / D)
        sq = None
        for k in range(PIECES):
            d = y[t, k].astype(F32) - mu
            sq = d * d if sq is None else sq + d * d
        rstd = lax.rsqrt(jnp.sum(sq, axis=-1, keepdims=True) * (1.0 / D) + EPS)
        for k in range(PIECES):
            cols = slice(k * DP, (k + 1) * DP)
            h[:, cols] = ((y[t, k].astype(F32) - mu) * rstd * g[:, cols]).astype(BF16)
        if first:
            own1.wait()
        for half in range(2):
            if first and half == 1:
                sib1.wait_recv()
            for j in range(H // TH):
                acc = jnp.dot(h[...], W1[half, :, j * TH:(j + 1) * TH], preferred_element_type=F32)
                a[:, half * H + j * TH:half * H + (j + 1) * TH] = _gelu(acc).astype(BF16)
        if first:
            own2.wait()
            sib2.wait_recv()
        for k in range(PIECES):
            if not first:
                finish(t - 1, k)
            cols = slice(k * DP, (k + 1) * DP)
            acc = jnp.dot(a[:, :H], W2[0, :, cols], preferred_element_type=F32)
            acc = acc + jnp.dot(a[:, H:], W2[1, :, cols], preferred_element_type=F32)
            p[t % 2, k] = acc.astype(BF16)
            p_copy(t, k).start()

    step(0, True)

    @pl.loop(1, N)
    def _(t):
        step(t, False)

    for k in range(PIECES):
        finish(N - 1, k)

    sib1.wait_send()
    sib2.wait_send()

    @pl.when(has_succ)
    def _():
        @pl.loop(0, N)
        def _(t):
            remote(y.at[t], y.at[t], y_send.at[t], y_sem.at[t], succ).wait_send()

    @pl.loop(0, per_rank)
    def _(i):
        pltpu.make_async_copy(y.at[i], y.at[i], o_sem.at[i]).wait()

        @pl.when(c == 1)
        def _():
            pltpu.make_async_copy(y.at[i], y.at[i], o_send.at[i]).wait()

        @pl.when((s == sender(i)) | ((s == 0) & (c == 1)))
        def _():
            pltpu.make_async_copy(y.at[i], y.at[i], in_send.at[i]).wait()


def solution(mesh):
    S = mesh.shape['stage']

    def local(x, g, w1, w2):
        M, TL, D = x.shape
        H = w1.shape[-1]
        N = 4 * M * (TL // CHUNK)
        DP = D // PIECES
        dma = pltpu.SemaphoreType.DMA
        return pl.pallas_call(
            functools.partial(_kernel, S, M, TL),
            out_shape=jax.ShapeDtypeStruct((1, M, TL, D), BF16),
            in_specs=[pl.BlockSpec(memory_space=pl.ANY), pl.BlockSpec(memory_space=pltpu.VMEM),
                      pl.BlockSpec(memory_space=pl.ANY), pl.BlockSpec(memory_space=pl.ANY)],
            out_specs=pl.BlockSpec(memory_space=pl.ANY),
            scratch_shapes=[
                pltpu.VMEM((2, D, H), BF16), pltpu.VMEM((2, H, D), BF16),
                pltpu.VMEM((N, PIECES, CHUNK, DP), BF16), pltpu.VMEM((N, PIECES, CHUNK, DP), BF16),
                pltpu.VMEM((2, PIECES, CHUNK, DP), BF16), pltpu.VMEM((CHUNK, D), BF16),
                pltpu.VMEM((CHUNK, 2 * H), BF16),
                dma((4,)), dma((2,)), dma((N,)), dma((N,)), dma((N, PIECES)), dma((2, PIECES)),
                dma((N // 4,)), dma((N // 4,)), dma((N // 4,)),
            ],
            compiler_params=pltpu.CompilerParams(has_side_effects=True, vmem_limit_bytes=67043328),
        )(x, g, w1, w2)

    return jax.shard_map(
        local, mesh=mesh,
        in_specs=(P(None, 'tp', None), P('stage', None, None),
                  P('stage', None, None, 'tp'), P('stage', None, 'tp', None)),
        out_specs=P('stage', None, 'tp', None), check_vma=False)
```

```python
import functools

import jax
import jax.numpy as jnp
from jax import lax
from jax.experimental import pallas as pl
from jax.experimental.pallas import tpu as pltpu
from jax.sharding import PartitionSpec as P

EPS = 1e-5
CHUNK = 64
ROWS = 128
PIECES = 4
ORDER = ('A0', 'A1', 'A2', 'A3', 'F0', 'F1', 'F2', 'T0', 'F3', 'T1', 'T2', 'T3')
MESH = pl.DeviceIdType.MESH
F32, BF16 = jnp.float32, jnp.bfloat16


def _gelu(v):
    return 0.5 * v * (1.0 + jnp.tanh(0.7978845608028654 * (v + 0.044715 * (v * v * v))))


def _kernel(S, M, TL, x_ref, g_ref, w1_ref, w2_ref, out_ref, W1, W2, y, xr, p, h, a,
            w_sem, w_send, y_sem, y_send, x_sem, p_send, o_sem, o_send, in_send):
    C = CHUNK
    s, r = lax.axis_index('stage'), lax.axis_index('tp')
    xp, c = r // 2, r % 2
    sub_n = TL // C
    per_rank = M * sub_n
    N = 4 * per_rank
    D = h.shape[1]
    DP = D // PIECES
    H = W1.shape[2]
    TH = min(512, H // 2)
    sib = (s, 2 * xp + 1 - c)
    partner = (s, 2 * (1 - xp) + c)
    succ = (s + c, 2 * xp + 1 - c)
    has_succ = 2 * s + c < 2 * S - 1

    def remote(src, dst, ss, rs, dev):
        return pltpu.make_async_remote_copy(src_ref=src, dst_ref=dst, send_sem=ss, recv_sem=rs,
                                            device_id=dev, device_id_type=MESH)

    own1 = pltpu.make_async_copy(w1_ref.at[0, c], W1.at[0], w_sem.at[0])
    own2 = pltpu.make_async_copy(w2_ref.at[0, c], W2.at[0], w_sem.at[2])
    sib1 = remote(w1_ref.at[0, 1 - c], W1.at[1], w_send.at[0], w_sem.at[1], sib)
    sib2 = remote(w2_ref.at[0, 1 - c], W2.at[1], w_send.at[1], w_sem.at[3], sib)
    own1.start()

    def x_piece(i, k):
        return x_ref.at[i // sub_n, pl.ds(pl.multiple_of((i % sub_n) * C, C), C), pl.ds(k * DP, DP)]

    def sender(i):
        return jnp.maximum(1, i * S // per_rank)

    @pl.when(s == 0)
    def _():
        @pl.loop(0, per_rank)
        def _(i):
            for k in range(PIECES):
                @pl.when(c == 0)
                def _():
                    pltpu.make_async_copy(x_piece(i, k), y.at[4 * i + r, k], y_sem.at[4 * i + r]).start()

                @pl.when(c == 1)
                def _():
                    remote(x_piece(i, k), y.at[4 * i + r, k], in_send.at[i], y_sem.at[4 * i + r], sib).start()

    @pl.when(s > 0)
    def _():
        @pl.loop(0, per_rank)
        def _(i):
            @pl.when(s == sender(i))
            def _():
                for k in range(PIECES):
                    remote(x_piece(i, k), y.at[4 * i + r, k], in_send.at[i], y_sem.at[4 * i + r],
                           (0, 2 * (1 - xp))).start()

    sib1.start()
    own2.start()
    sib2.start()

    g = jnp.where(c == 0, g_ref[0, 0:1, :].astype(F32), g_ref[0, 1:2, :].astype(F32))

    def p_copy(t, k):
        return remote(p.at[t % 2, k], xr.at[t, k], p_send.at[t % 2, k], x_sem.at[t, k], partner)

    def out_piece(t, k):
        i = t // 4
        return out_ref.at[0, i // sub_n, pl.ds(pl.multiple_of((i % sub_n) * C, C), C), pl.ds(k * DP, DP)]

    def finish(t, k):
        copy = p_copy(t, k)
        copy.wait_recv()
        v = y[t, k].astype(F32) + (p[t % 2, k].astype(F32) + xr[t, k].astype(F32))
        y[t, k] = v.astype(BF16)

        @pl.when(has_succ)
        def _():
            remote(y.at[t, k], y.at[t, k], y_send.at[t], y_sem.at[t], succ).start()

        copy.wait_send()

    def put_out(t):
        mine = (c == 1) & ((t % 4) // 2 == xp)

        @pl.when(mine & (t % 2 == 1))
        def _():
            for k in range(PIECES):
                pltpu.make_async_copy(y.at[t, k], out_piece(t, k), o_sem.at[t // 4]).start()

        @pl.when(mine & (t % 2 == 0))
        def _():
            for k in range(PIECES):
                remote(y.at[t, k], out_piece(t, k), o_send.at[t // 4], o_sem.at[t // 4], sib).start()

    def step(t, first):
        pltpu.make_async_copy(y.at[t], y.at[t], y_sem.at[t]).wait()
        tot = y[t, 0].astype(F32)
        for k in range(1, PIECES):
            tot = tot + y[t, k].astype(F32)
        mu = jnp.sum(tot, axis=-1, keepdims=True) * (1.0 / D)
        sq = None
        for k in range(PIECES):
            d = y[t, k].astype(F32) - mu
            sq = d * d if sq is None else sq + d * d
        rstd = lax.rsqrt(jnp.sum(sq, axis=-1, keepdims=True) * (1.0 / D) + EPS)
        for k in range(PIECES):
            cols = slice(k * DP, (k + 1) * DP)
            h[:C, cols] = ((y[t, k].astype(F32) - mu) * rstd * g[:, cols]).astype(BF16)
        for op in ORDER:
            kind, k = op[0], int(op[1:])
            if kind == 'A':
                if first and k == 0:
                    own1.wait()
                if first and k == 2:
                    sib1.wait_recv()
                Q = H // 2
                for j in range(0, Q, TH):
                    o = (k % 2) * Q + j
                    acc = jnp.dot(h[...], W1[k // 2, :, o:o + TH], preferred_element_type=F32)
                    a[:C, k * Q + j:k * Q + j + TH] = _gelu(acc[:C]).astype(BF16)
            elif kind == 'F':
                if not first:
                    finish(t - 1, k)
            else:
                if first and k == 0:
                    own2.wait()
                    sib2.wait_recv()
                TN = min(512, DP)
                for j in range(0, DP, TN):
                    o = k * DP + j
                    acc = jnp.dot(a[:, :H], W2[0, :, o:o + TN], preferred_element_type=F32)
                    acc = acc + jnp.dot(a[:, H:], W2[1, :, o:o + TN], preferred_element_type=F32)
                    p[t % 2, k, :, j:j + TN] = acc[:C].astype(BF16)
                p_copy(t, k).start()
        if not first:
            put_out(t - 1)

    h[C:, :] = jnp.zeros((ROWS - C, D), BF16)
    a[C:, :] = jnp.zeros((ROWS - C, 2 * H), BF16)
    step(0, True)

    @pl.loop(1, N)
    def _(t):
        step(t, False)

    for k in range(PIECES):
        finish(N - 1, k)
    put_out(N - 1)

    sib1.wait_send()
    sib2.wait_send()

    @pl.when(has_succ)
    def _():
        @pl.loop(0, N)
        def _(t):
            remote(y.at[t], y.at[t], y_send.at[t], y_sem.at[t], succ).wait_send()

    @pl.loop(0, per_rank)
    def _(i):
        pltpu.make_async_copy(y.at[i], y.at[i], o_sem.at[i]).wait()

        @pl.when(c == 1)
        def _():
            pltpu.make_async_copy(y.at[i], y.at[i], o_send.at[i]).wait()

        @pl.when((s == sender(i)) | ((s == 0) & (c == 1)))
        def _():
            pltpu.make_async_copy(y.at[i], y.at[i], in_send.at[i]).wait()


def solution(mesh):
    S = mesh.shape['stage']

    def local(x, g, w1, w2):
        M, TL, D = x.shape
        H = w1.shape[-1]
        N = 4 * M * (TL // CHUNK)
        DP = D // PIECES
        dma = pltpu.SemaphoreType.DMA
        return pl.pallas_call(
            functools.partial(_kernel, S, M, TL),
            out_shape=jax.ShapeDtypeStruct((1, M, TL, D), BF16),
            in_specs=[pl.BlockSpec(memory_space=pl.ANY), pl.BlockSpec(memory_space=pltpu.VMEM),
                      pl.BlockSpec(memory_space=pl.ANY), pl.BlockSpec(memory_space=pl.ANY)],
            out_specs=pl.BlockSpec(memory_space=pl.ANY),
            scratch_shapes=[
                pltpu.VMEM((2, D, H), BF16), pltpu.VMEM((2, H, D), BF16),
                pltpu.VMEM((N, PIECES, CHUNK, DP), BF16), pltpu.VMEM((N, PIECES, CHUNK, DP), BF16),
                pltpu.VMEM((2, PIECES, CHUNK, DP), BF16), pltpu.VMEM((ROWS, D), BF16),
                pltpu.VMEM((ROWS, 2 * H), BF16),
                dma((4,)), dma((2,)), dma((N,)), dma((N,)), dma((N, PIECES)), dma((2, PIECES)),
                dma((N // 4,)), dma((N // 4,)), dma((N // 4,)),
            ],
            compiler_params=pltpu.CompilerParams(has_side_effects=True, vmem_limit_bytes=67043328),
        )(x, g, w1, w2)

    return jax.shard_map(
        local, mesh=mesh,
        in_specs=(P(None, 'tp', None), P('stage', None, None),
                  P('stage', None, None, 'tp'), P('stage', None, 'tp', None)),
        out_specs=P('stage', None, 'tp', None), check_vma=False)
```

```python
import functools

import jax
import jax.numpy as jnp
from jax import lax
from jax.experimental import pallas as pl
from jax.experimental.pallas import tpu as pltpu
from jax.sharding import PartitionSpec as P

EPS = 1e-5
CHUNK = 64
ROWS = 128
PIECES = 4
ORDER = ('A0', 'A1', 'A2', 'F0', 'F1', 'A3', 'F2', 'F3', 'T0', 'T1', 'T2', 'T3')
MESH = pl.DeviceIdType.MESH
F32, BF16 = jnp.float32, jnp.bfloat16


def _gelu(v):
    return 0.5 * v * (1.0 + jnp.tanh(0.7978845608028654 * (v + 0.044715 * (v * v * v))))


def _kernel(S, M, TL, x_ref, g_ref, w1_ref, w2_ref, out_ref, W1, W2, y, xr, p, h, a,
            w_sem, w_send, y_sem, y_send, x_sem, p_send, o_sem, o_send, in_send):
    C = CHUNK
    s, r = lax.axis_index('stage'), lax.axis_index('tp')
    xp, c = r // 2, r % 2
    sub_n = TL // C
    per_rank = M * sub_n
    N = 4 * per_rank
    D = h.shape[1]
    DP = D // PIECES
    H = W1.shape[2]
    TH = min(512, H // 2)
    sib = (s, 2 * xp + 1 - c)
    partner = (s, 2 * (1 - xp) + c)
    succ = (s + c, 2 * xp + 1 - c)
    has_succ = 2 * s + c < 2 * S - 1

    def remote(src, dst, ss, rs, dev):
        return pltpu.make_async_remote_copy(src_ref=src, dst_ref=dst, send_sem=ss, recv_sem=rs,
                                            device_id=dev, device_id_type=MESH)

    own1 = pltpu.make_async_copy(w1_ref.at[0, c], W1.at[0], w_sem.at[0])
    own2 = pltpu.make_async_copy(w2_ref.at[0, c], W2.at[0], w_sem.at[2])
    sib1 = remote(w1_ref.at[0, 1 - c], W1.at[1], w_send.at[0], w_sem.at[1], sib)
    sib2 = [remote(w2_ref.at[0, 1 - c, :, pl.ds(k * DP, DP)], W2.at[1, :, pl.ds(k * DP, DP)],
                   w_send.at[1 + k], w_sem.at[3 + k], sib) for k in range(PIECES)]
    own1.start()
    own2.start()

    barrier = pltpu.get_barrier_semaphore()

    def greet(dev):
        pl.semaphore_signal(barrier, inc=1, device_id=dev, device_id_type=MESH)

    greet(sib)
    greet(partner)

    @pl.when((c == 0) & (s > 0))
    def _():
        greet((s - 1, 2 * xp + 1))

    @pl.when((c == 0) & (s == 0))
    def _():
        @pl.loop(1, S)
        def _(i):
            greet((i, 2 * (1 - xp)))
            greet((i, 2 * (1 - xp) + 1))

    pl.semaphore_wait(barrier, 2 + jnp.minimum(s, 1) + c * jnp.minimum(S - 1 - s, 1))

    sib1.start()
    for cp in sib2:
        cp.start()

    def x_piece(i, k):
        return x_ref.at[i // sub_n, pl.ds(pl.multiple_of((i % sub_n) * C, C), C), pl.ds(k * DP, DP)]

    def sender(i):
        return jnp.maximum(1, i * S // per_rank)

    @pl.when(s == 0)
    def _():
        @pl.loop(0, per_rank)
        def _(i):
            for k in range(PIECES):
                @pl.when(c == 0)
                def _():
                    pltpu.make_async_copy(x_piece(i, k), y.at[4 * i + r, k], y_sem.at[4 * i + r]).start()

                @pl.when(c == 1)
                def _():
                    remote(x_piece(i, k), y.at[4 * i + r, k], in_send.at[i], y_sem.at[4 * i + r], sib).start()

    @pl.when(s > 0)
    def _():
        @pl.loop(0, per_rank)
        def _(i):
            @pl.when(s == sender(i))
            def _():
                for k in range(PIECES):
                    remote(x_piece(i, k), y.at[4 * i + r, k], in_send.at[i], y_sem.at[4 * i + r],
                           (0, 2 * (1 - xp))).start()

    g = jnp.where(c == 0, g_ref[0, 0:1, :].astype(F32), g_ref[0, 1:2, :].astype(F32))

    def p_copy(t, k):
        return remote(p.at[t % 2, k], xr.at[t, k], p_send.at[t % 2, k], x_sem.at[t, k], partner)

    def out_piece(t, k):
        i = t // 4
        return out_ref.at[0, i // sub_n, pl.ds(pl.multiple_of((i % sub_n) * C, C), C), pl.ds(k * DP, DP)]

    def finish(t, k):
        copy = p_copy(t, k)
        copy.wait_recv()
        v = y[t, k].astype(F32) + (p[t % 2, k].astype(F32) + xr[t, k].astype(F32))
        y[t, k] = v.astype(BF16)

        @pl.when(has_succ)
        def _():
            remote(y.at[t, k], y.at[t, k], y_send.at[t], y_sem.at[t], succ).start()

        copy.wait_send()

    def put_out(t):
        mine = (c == 1) & ((t % 4) // 2 == xp)

        @pl.when(mine & (t % 2 == 1))
        def _():
            for k in range(PIECES):
                pltpu.make_async_copy(y.at[t, k], out_piece(t, k), o_sem.at[t // 4]).start()

        @pl.when(mine & (t % 2 == 0))
        def _():
            for k in range(PIECES):
                remote(y.at[t, k], out_piece(t, k), o_send.at[t // 4], o_sem.at[t // 4], sib).start()

    def step(t, first):
        pltpu.make_async_copy(y.at[t], y.at[t], y_sem.at[t]).wait()
        tot = y[t, 0].astype(F32)
        for k in range(1, PIECES):
            tot = tot + y[t, k].astype(F32)
        mu = jnp.sum(tot, axis=-1, keepdims=True) * (1.0 / D)
        sq = None
        for k in range(PIECES):
            d = y[t, k].astype(F32) - mu
            sq = d * d if sq is None else sq + d * d
        rstd = lax.rsqrt(jnp.sum(sq, axis=-1, keepdims=True) * (1.0 / D) + EPS)
        for k in range(PIECES):
            cols = slice(k * DP, (k + 1) * DP)
            h[:C, cols] = ((y[t, k].astype(F32) - mu) * rstd * g[:, cols]).astype(BF16)
        for op in ORDER:
            kind, k = op[0], int(op[1:])
            if kind == 'A':
                if first and k == 0:
                    own1.wait()
                if first and k == 2:
                    sib1.wait_recv()
                Q = H // 2
                for j in range(0, Q, TH):
                    o = (k % 2) * Q + j
                    acc = jnp.dot(h[...], W1[k // 2, :, o:o + TH], preferred_element_type=F32)
                    a[:C, k * Q + j:k * Q + j + TH] = _gelu(acc[:C]).astype(BF16)
            elif kind == 'F':
                if not first:
                    finish(t - 1, k)
            else:
                if first and k == 0:
                    own2.wait()
                if first:
                    sib2[k].wait_recv()
                TN = min(512, DP)
                for j in range(0, DP, TN):
                    o = k * DP + j
                    acc = jnp.dot(a[:, :H], W2[0, :, o:o + TN], preferred_element_type=F32)
                    acc = acc + jnp.dot(a[:, H:], W2[1, :, o:o + TN], preferred_element_type=F32)
                    p[t % 2, k, :, j:j + TN] = acc[:C].astype(BF16)
                p_copy(t, k).start()
        if not first:
            put_out(t - 1)

    h[C:, :] = jnp.zeros((ROWS - C, D), BF16)
    a[C:, :] = jnp.zeros((ROWS - C, 2 * H), BF16)
    step(0, True)

    @pl.loop(1, N)
    def _(t):
        step(t, False)

    for k in range(PIECES):
        finish(N - 1, k)
    put_out(N - 1)

    sib1.wait_send()
    for cp in sib2:
        cp.wait_send()

    @pl.when(has_succ)
    def _():
        @pl.loop(0, N)
        def _(t):
            remote(y.at[t], y.at[t], y_send.at[t], y_sem.at[t], succ).wait_send()

    @pl.loop(0, per_rank)
    def _(i):
        pltpu.make_async_copy(y.at[i], y.at[i], o_sem.at[i]).wait()

        @pl.when(c == 1)
        def _():
            pltpu.make_async_copy(y.at[i], y.at[i], o_send.at[i]).wait()

        @pl.when((s == sender(i)) | ((s == 0) & (c == 1)))
        def _():
            pltpu.make_async_copy(y.at[i], y.at[i], in_send.at[i]).wait()


def solution(mesh):
    S = mesh.shape['stage']

    def local(x, g, w1, w2):
        M, TL, D = x.shape
        H = w1.shape[-1]
        N = 4 * M * (TL // CHUNK)
        DP = D // PIECES
        dma = pltpu.SemaphoreType.DMA
        return pl.pallas_call(
            functools.partial(_kernel, S, M, TL),
            out_shape=jax.ShapeDtypeStruct((1, M, TL, D), BF16),
            in_specs=[pl.BlockSpec(memory_space=pl.ANY), pl.BlockSpec(memory_space=pltpu.VMEM),
                      pl.BlockSpec(memory_space=pl.ANY), pl.BlockSpec(memory_space=pl.ANY)],
            out_specs=pl.BlockSpec(memory_space=pl.ANY),
            scratch_shapes=[
                pltpu.VMEM((2, D, H), BF16), pltpu.VMEM((2, H, D), BF16),
                pltpu.VMEM((N, PIECES, CHUNK, DP), BF16), pltpu.VMEM((N, PIECES, CHUNK, DP), BF16),
                pltpu.VMEM((2, PIECES, CHUNK, DP), BF16), pltpu.VMEM((ROWS, D), BF16),
                pltpu.VMEM((ROWS, 2 * H), BF16),
                dma((3 + PIECES,)), dma((1 + PIECES,)), dma((N,)), dma((N,)), dma((N, PIECES)), dma((2, PIECES)),
                dma((N // 4,)), dma((N // 4,)), dma((N // 4,)),
            ],
            compiler_params=pltpu.CompilerParams(collective_id=0, has_side_effects=True, vmem_limit_bytes=67043328),
        )(x, g, w1, w2)

    return jax.shard_map(
        local, mesh=mesh,
        in_specs=(P(None, 'tp', None), P('stage', None, None),
                  P('stage', None, None, 'tp'), P('stage', None, 'tp', None)),
        out_specs=P('stage', None, 'tp', None), check_vma=False)
```

```python
import functools

import jax
import jax.numpy as jnp
from jax import lax
from jax.experimental import pallas as pl
from jax.experimental.pallas import tpu as pltpu
from jax.sharding import PartitionSpec as P

EPS = 1e-5
CHUNK = 64
ROWS = 128
PIECES = 4
ORDER = ('A0', 'A1', 'A2', 'F0', 'F1', 'A3', 'F2', 'F3', 'T0', 'T1', 'T2', 'T3')
MESH = pl.DeviceIdType.MESH
F32, BF16 = jnp.float32, jnp.bfloat16


def _gelu(v):
    return 0.5 * v * (1.0 + jnp.tanh(0.7978845608028654 * (v + 0.044715 * (v * v * v))))


def _kernel(S, M, TL, x_ref, g_ref, w1_ref, w2_ref, out_ref, W1, W2, y, xr, p, h, a,
            w_sem, w_send, y_sem, y_send, x_sem, p_send, o_sem, o_send, in_send):
    C = CHUNK
    s, r = lax.axis_index('stage'), lax.axis_index('tp')
    xp, c = r // 2, r % 2
    sub_n = TL // C
    per_rank = M * sub_n
    N = 4 * per_rank
    D = h.shape[1]
    DP = D // PIECES
    H = W1.shape[2]
    TH = min(512, H // 2)
    sib = (s, 2 * xp + 1 - c)
    partner = (s, 2 * (1 - xp) + c)
    succ = (s + c, 2 * xp + 1 - c)
    has_succ = 2 * s + c < 2 * S - 1

    def remote(src, dst, ss, rs, dev):
        return pltpu.make_async_remote_copy(src_ref=src, dst_ref=dst, send_sem=ss, recv_sem=rs,
                                            device_id=dev, device_id_type=MESH)

    own1 = pltpu.make_async_copy(w1_ref.at[0, c], W1.at[0], w_sem.at[0])
    own2 = pltpu.make_async_copy(w2_ref.at[0, c], W2.at[0], w_sem.at[2])
    sib1 = remote(w1_ref.at[0, 1 - c], W1.at[1], w_send.at[0], w_sem.at[1], sib)
    sib2 = [remote(w2_ref.at[0, 1 - c, :, pl.ds(k * DP, DP)], W2.at[1, :, pl.ds(k * DP, DP)],
                   w_send.at[1 + k], w_sem.at[3 + k], sib) for k in range(PIECES)]
    own1.start()
    own2.start()

    barrier = pltpu.get_barrier_semaphore()

    def greet(dev):
        pl.semaphore_signal(barrier, inc=1, device_id=dev, device_id_type=MESH)

    greet(sib)
    greet(partner)

    @pl.when((c == 0) & (s > 0))
    def _():
        greet((s - 1, 2 * xp + 1))

    @pl.when((c == 0) & (s == 0))
    def _():
        @pl.loop(1, S)
        def _(i):
            greet((i, 2 * (1 - xp)))
            greet((i, 2 * (1 - xp) + 1))

    pl.semaphore_wait(barrier, 2 + jnp.minimum(s, 1) + c * jnp.minimum(S - 1 - s, 1))

    sib1.start()
    for cp in sib2:
        cp.start()

    def x_piece(i, k):
        return x_ref.at[i // sub_n, pl.ds(pl.multiple_of((i % sub_n) * C, C), C), pl.ds(k * DP, DP)]

    def sender(i):
        return jnp.maximum(1, i * S // per_rank)

    @pl.when(s == 0)
    def _():
        @pl.loop(0, per_rank)
        def _(i):
            for k in range(PIECES):
                @pl.when(c == 0)
                def _():
                    pltpu.make_async_copy(x_piece(i, k), y.at[4 * i + r, k], y_sem.at[4 * i + r]).start()

                @pl.when(c == 1)
                def _():
                    remote(x_piece(i, k), y.at[4 * i + r, k], in_send.at[i], y_sem.at[4 * i + r], sib).start()

    @pl.when(s > 0)
    def _():
        @pl.loop(0, per_rank)
        def _(i):
            @pl.when(s == sender(i))
            def _():
                for k in range(PIECES):
                    remote(x_piece(i, k), y.at[4 * i + r, k], in_send.at[i], y_sem.at[4 * i + r],
                           (0, 2 * (1 - xp))).start()

    g = jnp.where(c == 0, g_ref[0, 0:1, :].astype(F32), g_ref[0, 1:2, :].astype(F32))

    def p_copy(t, k):
        return remote(p.at[t % 2, k], xr.at[t, k], p_send.at[t % 2, k], x_sem.at[t, k], partner)

    def out_piece(t, k):
        i = t // 4
        return out_ref.at[0, i // sub_n, pl.ds(pl.multiple_of((i % sub_n) * C, C), C), pl.ds(k * DP, DP)]

    def finish(t, k):
        p_copy(t, k).wait_recv()
        v = y[t, k].astype(F32) + (p[t % 2, k].astype(F32) + xr[t, k].astype(F32))
        y[t, k] = v.astype(BF16)

        @pl.when(has_succ)
        def _():
            remote(y.at[t, k], y.at[t, k], y_send.at[t], y_sem.at[t], succ).start()

    def put_out(t):
        for k in range(PIECES):
            p_copy(t, k).wait_send()
        mine = (c == 1) & ((t % 4) // 2 == xp)

        @pl.when(mine & (t % 2 == 1))
        def _():
            for k in range(PIECES):
                pltpu.make_async_copy(y.at[t, k], out_piece(t, k), o_sem.at[t // 4]).start()

        @pl.when(mine & (t % 2 == 0))
        def _():
            for k in range(PIECES):
                remote(y.at[t, k], out_piece(t, k), o_send.at[t // 4], o_sem.at[t // 4], sib).start()

    def step(t, first):
        pltpu.make_async_copy(y.at[t], y.at[t], y_sem.at[t]).wait()
        tot = y[t, 0].astype(F32)
        for k in range(1, PIECES):
            tot = tot + y[t, k].astype(F32)
        mu = jnp.sum(tot, axis=-1, keepdims=True) * (1.0 / D)
        sq = None
        for k in range(PIECES):
            d = y[t, k].astype(F32) - mu
            sq = d * d if sq is None else sq + d * d
        rstd = lax.rsqrt(jnp.sum(sq, axis=-1, keepdims=True) * (1.0 / D) + EPS)
        for k in range(PIECES):
            cols = slice(k * DP, (k + 1) * DP)
            h[:C, cols] = ((y[t, k].astype(F32) - mu) * rstd * g[:, cols]).astype(BF16)
        for op in ORDER:
            kind, k = op[0], int(op[1:])
            if kind == 'A':
                if first and k == 0:
                    own1.wait()
                if first and k == 2:
                    sib1.wait_recv()
                Q = H // 2
                for j in range(0, Q, TH):
                    o = (k % 2) * Q + j
                    acc = jnp.dot(h[...], W1[k // 2, :, o:o + TH], preferred_element_type=F32)
                    a[:C, k * Q + j:k * Q + j + TH] = _gelu(acc[:C]).astype(BF16)
            elif kind == 'F':
                if not first:
                    finish(t - 1, k)
            else:
                if first and k == 0:
                    own2.wait()
                if first:
                    sib2[k].wait_recv()
                TN = min(512, DP)
                for j in range(0, DP, TN):
                    o = k * DP + j
                    acc = jnp.dot(a[:, :H], W2[0, :, o:o + TN], preferred_element_type=F32)
                    acc = acc + jnp.dot(a[:, H:], W2[1, :, o:o + TN], preferred_element_type=F32)
                    p[t % 2, k, :, j:j + TN] = acc[:C].astype(BF16)
                p_copy(t, k).start()
        if not first:
            put_out(t - 1)

    h[C:, :] = jnp.zeros((ROWS - C, D), BF16)
    a[C:, :] = jnp.zeros((ROWS - C, 2 * H), BF16)
    step(0, True)

    @pl.loop(1, N)
    def _(t):
        step(t, False)

    for k in range(PIECES):
        finish(N - 1, k)
    put_out(N - 1)

    sib1.wait_send()
    for cp in sib2:
        cp.wait_send()

    @pl.when(has_succ)
    def _():
        @pl.loop(0, N)
        def _(t):
            remote(y.at[t], y.at[t], y_send.at[t], y_sem.at[t], succ).wait_send()

    @pl.loop(0, per_rank)
    def _(i):
        pltpu.make_async_copy(y.at[i], y.at[i], o_sem.at[i]).wait()

        @pl.when(c == 1)
        def _():
            pltpu.make_async_copy(y.at[i], y.at[i], o_send.at[i]).wait()

        @pl.when((s == sender(i)) | ((s == 0) & (c == 1)))
        def _():
            pltpu.make_async_copy(y.at[i], y.at[i], in_send.at[i]).wait()


def solution(mesh):
    S = mesh.shape['stage']

    def local(x, g, w1, w2):
        M, TL, D = x.shape
        H = w1.shape[-1]
        N = 4 * M * (TL // CHUNK)
        DP = D // PIECES
        dma = pltpu.SemaphoreType.DMA
        return pl.pallas_call(
            functools.partial(_kernel, S, M, TL),
            out_shape=jax.ShapeDtypeStruct((1, M, TL, D), BF16),
            in_specs=[pl.BlockSpec(memory_space=pl.ANY), pl.BlockSpec(memory_space=pltpu.VMEM),
                      pl.BlockSpec(memory_space=pl.ANY), pl.BlockSpec(memory_space=pl.ANY)],
            out_specs=pl.BlockSpec(memory_space=pl.ANY),
            scratch_shapes=[
                pltpu.VMEM((2, D, H), BF16), pltpu.VMEM((2, H, D), BF16),
                pltpu.VMEM((N, PIECES, CHUNK, DP), BF16), pltpu.VMEM((N, PIECES, CHUNK, DP), BF16),
                pltpu.VMEM((2, PIECES, CHUNK, DP), BF16), pltpu.VMEM((ROWS, D), BF16),
                pltpu.VMEM((ROWS, 2 * H), BF16),
                dma((3 + PIECES,)), dma((1 + PIECES,)), dma((N,)), dma((N,)), dma((N, PIECES)), dma((2, PIECES)),
                dma((N // 4,)), dma((N // 4,)), dma((N // 4,)),
            ],
            compiler_params=pltpu.CompilerParams(collective_id=0, has_side_effects=True, vmem_limit_bytes=67043328),
        )(x, g, w1, w2)

    return jax.shard_map(
        local, mesh=mesh,
        in_specs=(P(None, 'tp', None), P('stage', None, None),
                  P('stage', None, None, 'tp'), P('stage', None, 'tp', None)),
        out_specs=P('stage', None, 'tp', None), check_vma=False)
```
